512 devices in a mesh: dp: 128 (over z_lo, x, y), mp: 4 (over z_hi, core).
Axes of the slice: x: 4, y: 8, z: 8 (z_hi: 2, z_lo: 4; z = z_hi * 4 + z_lo), core: 2. Of those that a mesh axis runs over, the one named last changes fastest.
Arguments:
- images: bfloat16 [24576, 1024], P('dp', 'mp'), may hold values from -80 to 80, as said below
- texts: bfloat16 [24576, 1024], P('dp', 'mp'), may hold values from -80 to 80, as said below
- logit_scale: float32 [1], replicated, may hold values from 240 to 300
Outputs:
- row_loss: float32 [24576], P('dp')
- column_loss: float32 [24576], P('dp')
The draws below stay inside these ranges and needn't reach their ends.
Inputs may be any that keep to these rules, and one draw needn't show every extreme that they name: `images`: Real-valued entries. `texts`: Real-valued entries.
All inputs are finite; a program needn't handle non-finite values.
Results may differ from the reference program's by a relative error of at most 0.0044.
Values may be sent and summed in bfloat16 or wider, within the bound.
A program may use at most 64 MiB of HBM per device.

```python
import jax
import jax.numpy as jnp
from jax import lax

D = 1024
ROWS_DEV = 192
BATCH = 24576
N_DP = 128


def draw_pair(key):
    image_key = jax.random.fold_in(key, 11)
    text_key = jax.random.fold_in(key, 12)
    common_key = jax.random.fold_in(key, 15)
    spread_key = jax.random.fold_in(key, 16)
    common = jax.random.normal(common_key, (1, D), jnp.float32)
    block_spread = jnp.exp(jax.random.uniform(spread_key, (BATCH // ROWS_DEV,), jnp.float32, jnp.log(0.03), 0.0))
    spread = block_spread[jnp.arange(BATCH) // ROWS_DEV][:, None]
    weight = jnp.sqrt(1.0 - spread * spread)
    image_rows = weight * common + spread * jax.random.normal(image_key, (BATCH, D), jnp.float32)
    text_rows = jax.random.normal(text_key, (BATCH, D), jnp.float32)
    image_rows = jnp.clip(image_rows, -80.0, 80.0)
    text_rows = jnp.clip(text_rows, -80.0, 80.0)
    return (image_rows, text_rows)


def draw_images(key, part):
    return draw_pair(key)[0].astype(jnp.bfloat16)


def draw_texts(key, part):
    return draw_pair(key)[1].astype(jnp.bfloat16)


def setup_inputs(seed: int = 0) -> dict:
    streams_of = jax.random.split(jax.random.key(seed), 4)
    return {
        "images": draw_images(jax.random.fold_in(streams_of[3], 71), 0),
        "texts": draw_texts(jax.random.fold_in(streams_of[3], 71), 0),
        "logit_scale": jnp.clip(jax.random.uniform(streams_of[2], (1,), jnp.float32, 240.0, 300.0), 240.0, 300.0),
    }


def normalize(rows):
    values = rows.astype(jnp.float32)
    return (values * lax.rsqrt(lax.optimization_barrier(jnp.sum(values * values, axis=1, keepdims=True)) + 1e-06)).astype(jnp.bfloat16)

def reference(images, texts, logit_scale):
    image_unit = normalize(images)
    text_unit = normalize(texts)
    inverse_temp = logit_scale[0]
    matched = inverse_temp * lax.optimization_barrier(jnp.sum(image_unit.astype(jnp.float32) * text_unit.astype(jnp.float32), axis=1))
    blocks = text_unit.reshape(N_DP, ROWS_DEV, D)

    def visit(states, block):
        row_top, row_total = states
        scores = inverse_temp * jnp.dot(block, image_unit.T, preferred_element_type=jnp.float32)
        column_top = lax.optimization_barrier(jnp.max(scores, axis=1))
        column_lse = column_top + jnp.log(lax.optimization_barrier(jnp.sum(jnp.exp(scores - column_top[:, None]), axis=1)))
        new_top = jnp.maximum(row_top, lax.optimization_barrier(jnp.max(scores, axis=0)))
        row_total = row_total * jnp.exp(row_top - new_top) + lax.optimization_barrier(jnp.sum(jnp.exp(scores - new_top[None, :]), axis=0))
        return ((new_top, row_total), column_lse)
    start = (jnp.full((BATCH,), -1e+30, jnp.float32), jnp.zeros((BATCH,), jnp.float32))
    (row_top, row_total), column_lse = lax.scan(visit, start, blocks)
    row_loss = row_top + jnp.log(row_total) - matched
    column_loss = column_lse.reshape(-1) - matched
    return (row_loss, column_loss)
```

```python
import functools
import heapq

import jax
import jax.numpy as jnp
from jax import lax
from jax.experimental import pallas as pl
from jax.experimental.pallas import tpu as pltpu
from jax.sharding import Mesh
from jax.sharding import PartitionSpec as P

AXES = ("zl", "x", "y", "zh", "c")
SIZES = (4, 4, 8, 2, 2)
RING = 8
CHUNKS = 3
LOG2E = 1.4426950408889634
LN2 = 0.6931471805599453
TAU, LAT = 0.7, 1.9


def steps_of(chunk, col):
    return (4, 3) if (chunk + col) % 2 else (3, 4)


def schedule(start, busy_up):
    free = {"up": start + busy_up, "down": start, "across": start}
    heap, out, n = [], [], 0

    def send(link, t, item):
        nonlocal n
        begin = max(t, free[link])
        free[link] = begin + TAU
        n += 1
        heapq.heappush(heap, (begin + TAU + LAT, n, item))
        return (link, item)

    def along(t, item):
        chunk, col, d = item
        up, down = steps_of(chunk, col)
        got = []
        if d <= 0 and -d < up:
            got.append(send("up", t, (chunk, col, d - 1)))
        if d >= 0 and d < down:
            got.append(send("down", t, (chunk, col, d + 1)))
        return got

    first = [send("across", start, (c, 1, 0)) for c in (2, 0, 1)]
    for c in (0, 1, 2):
        first += along(start, (c, 0, 0))
    out.append((start, None, first))
    while heap:
        t, _, item = heapq.heappop(heap)
        chunk, col, d = item
        sends = []
        if chunk == 2:
            sends += along(t, item)
        elif col == 0:
            sends += along(t, item)
            sends.append(send("across", t, (chunk, 1, d)))
        out.append((t, item, sends))
    return out


IMAGE_PLAN = schedule(0.0, 2.0)
TEXT_PLAN = schedule(5.0, 0.0)
ITEMS = [item for _, item, _ in IMAGE_PLAN if item is not None]
INDEX = {item: i for i, item in enumerate(ITEMS)}
OWN = [(c, 0, 0) for c in range(CHUNKS)]
ALL = OWN + ITEMS
ALL_INDEX = {item: i for i, item in enumerate(ALL)}


def body(
    images_ref, texts_ref, scale_ref, row_ref, col_ref,
    img, txt, tq, raw, rowbuf, rs, rr, cs, cr, fin_src, fin,
    load_sem, a2a_send, a2a_recv, i_send, i_recv, t_send, t_recv, d_send, d_recv,
    r_send, r_recv, c_send, c_recv, f_send, f_recv,
):
    zl, x, y, zh, c = (lax.axis_index(a) for a in AXES)
    z = zh * 4 + zl
    m = zh * 2 + c
    odd = lax.rem(x, 2)
    xf = x + 1 - 2 * odd
    xg = lax.rem(x + 3 + 2 * odd, 4)
    other = 1 - c

    def at_z(pos):
        return {"zl": lax.rem(pos, 4), "zh": lax.div(pos, 4)}

    def ring(pos, d):
        return lax.rem(pos + (d + RING), RING)

    own_image = (zl * 2 + odd, m)
    own_text = y * 2 + (1 - odd)
    loads = [
        pltpu.make_async_copy(texts_ref, tq, load_sem.at[0]),
        pltpu.make_async_copy(texts_ref.at[m], raw.at[m], load_sem.at[1]),
        pltpu.make_async_copy(images_ref, img.at[own_image[0], own_image[1]], load_sem.at[2]),
    ]
    for load in loads:
        load.start()

    mp_peers = [(dz, dc) for dz in (0, 1) for dc in (0, 1) if dz or dc]

    def mp_of(dz, dc):
        return {"zh": (1 - zh) if dz else zh, "c": other if dc else c}

    links_image = {"up": at_z(ring(z, 1)), "down": at_z(ring(z, -1)), "across": {"x": xf}}
    links_text = {"up": {"y": ring(y, 1)}, "down": {"y": ring(y, -1)}, "across": {"x": xg}}
    barrier = pltpu.get_barrier_semaphore()
    peers = list(links_image.values()) + list(links_text.values()) + [mp_of(*p) for p in mp_peers]
    for peer in peers:
        pl.semaphore_signal(barrier, inc=1, device_id=peer, device_id_type=pl.DeviceIdType.MESH)
    for load in loads:
        load.wait()
    pl.semaphore_wait(barrier, len(peers))

    started = []

    def push(src, dst, send, recv, peer):
        copy = pltpu.make_async_remote_copy(
            src_ref=src, dst_ref=dst, send_sem=send, recv_sem=recv,
            device_id=peer, device_id_type=pl.DeviceIdType.MESH,
        )
        copy.start()
        started.append(copy)
        return copy

    swaps = []
    for n, (dz, dc) in enumerate(mp_peers):
        peer = mp_of(dz, dc)
        theirs = peer["zh"] * 2 + peer["c"]
        swaps.append(push(tq.at[theirs], raw.at[m], a2a_send.at[n], a2a_recv.at[n], peer))

    def image_slot(item, core):
        chunk, col, d = item
        pos = ring(z, d)
        block = lax.rem(pos, 4) * 2 + ((1 - odd) if col else odd)
        return img.at[block, lax.div(pos, 4) * 2 + core, chunk]

    def text_slot(item):
        chunk, col, d = item
        return txt.at[ring(y, d) * 2 + (odd if col else 1 - odd), chunk]

    def moved(link, item):
        chunk, col, d = item
        if link == "across":
            return (chunk, 1 - col, d)
        return (chunk, col, d + 1 if link == "up" else d - 1)

    def hand_over(item):
        n = ALL_INDEX[item]
        push(image_slot(item, c), image_slot(item, c), d_send.at[n], d_recv.at[n], {"c": other})

    def image_event(item, sends):
        if item is not None:
            slot = image_slot(item, c)
            n = INDEX[item]
            pltpu.make_async_remote_copy(
                src_ref=slot, dst_ref=slot, send_sem=i_send.at[n], recv_sem=i_recv.at[n],
                device_id={"c": other}, device_id_type=pl.DeviceIdType.MESH,
            ).wait_recv()
        for link, sent in sends:
            slot = image_slot(moved(link, sent), c)
            n = INDEX[sent]
            push(slot, slot, i_send.at[n], i_recv.at[n], links_image[link])
        for each in [item] if item is not None else OWN:
            hand_over(each)

    def text_event(item, sends):
        if item is not None:
            slot = text_slot(item)
            n = INDEX[item]
            pltpu.make_async_remote_copy(
                src_ref=slot, dst_ref=slot, send_sem=t_send.at[n], recv_sem=t_recv.at[n],
                device_id={"c": other}, device_id_type=pl.DeviceIdType.MESH,
            ).wait_recv()
        else:
            for swap in swaps:
                swap.wait_recv()
            rows = jnp.concatenate([raw[k] for k in range(4)], axis=1).astype(jnp.float32)
            unit = rows * lax.rsqrt(jnp.sum(rows * rows, axis=1, keepdims=True) + 1e-6)
            txt[own_text] = unit.astype(jnp.bfloat16).reshape(CHUNKS, 16, 1024)
        for link, sent in sends:
            slot = text_slot(moved(link, sent))
            n = INDEX[sent]
            push(slot, slot, t_send.at[n], t_recv.at[n], links_text[link])

    events = [(t, 0, n, item, sends) for n, (t, item, sends) in enumerate(IMAGE_PLAN)]
    events += [(t, 1, n, item, sends) for n, (t, item, sends) in enumerate(TEXT_PLAN)]
    for t, kind, _, item, sends in sorted(events, key=lambda e: e[:3]):
        (text_event if kind else image_event)(item, sends)
    for item in ALL:
        slot = image_slot(item, other)
        n = ALL_INDEX[item]
        pltpu.make_async_remote_copy(
            src_ref=slot, dst_ref=slot, send_sem=d_send.at[n], recv_sem=d_recv.at[n],
            device_id={"c": other}, device_id_type=pl.DeviceIdType.MESH,
        ).wait_recv()

    scale = scale_ref[0]

    def rows_of(block):
        parts = [img[block, q].reshape(192, 256) for q in range(4)]
        return jnp.concatenate(parts, axis=1)

    def visit(block, state):
        top, total = state
        rows = rows_of(block)
        wide = rows.astype(jnp.float32)
        factor = lax.rsqrt(jnp.sum(wide * wide, axis=1, keepdims=True) + 1e-6) * (scale * LOG2E)
        scores = factor * lax.dot_general(
            rows, txt[...].reshape(768, 1024), (((1,), (1,)), ((), ())), preferred_element_type=jnp.float32
        )
        row_top = jnp.max(scores, axis=1, keepdims=True)
        row_total = jnp.sum(jnp.exp2(scores - row_top), axis=1, keepdims=True)
        lane = lax.broadcasted_iota(jnp.int32, (192, 128), 1)
        rowbuf[pl.ds(pl.multiple_of(block * 192, 192), 192), :] = jnp.where(lane == 0, row_top, row_total)
        new = jnp.maximum(top, jnp.max(scores, axis=0, keepdims=True))
        total = total * jnp.exp2(top - new) + jnp.sum(jnp.exp2(scores - new), axis=0, keepdims=True)
        return (new, total)

    start = (jnp.full((1, 768), -1e30, jnp.float32), jnp.zeros((1, 768), jnp.float32))
    col_top, col_total = lax.fori_loop(0, 8, visit, start)

    for tb in range(16):
        shift = (768 - tb * 48) % 768
        for k, part in enumerate((col_top, col_total)):
            turned = pltpu.roll(part, shift, 1) if shift else part
            cs[tb, pl.ds(k, 1), :] = turned[:, :128]
    for dy in range(RING):
        for dx in (0, 1):
            n = dy * 2 + dx
            target = ring(y, dy) * 2 + (odd if dx else 1 - odd)
            if n == 0:
                cr[0] = cs[own_text]
            else:
                push(cs.at[target], cr.at[n], c_send.at[n], c_recv.at[n], {"y": ring(y, dy), "x": xg if dx else x})
    for k in range(12):
        turned = jnp.transpose(rowbuf[k * 128 : (k + 1) * 128, :])
        rs[k // 3, :, pl.ds((k % 3) * 128, 128)] = turned[0:2, :]
    for dz in range(RING):
        for dx in (0, 1):
            for dc in (0, 1):
                n = dz * 4 + dx * 2 + dc
                pos = ring(z, dz)
                if n == 0:
                    rr[0] = rs[zl]
                else:
                    push(
                        rs.at[lax.rem(pos, 4)], rr.at[n], r_send.at[n], r_recv.at[n],
                        {**at_z(pos), "x": xf if dx else x, "c": other if dc else c},
                    )

    mine = jnp.concatenate([img[own_image[0], q].reshape(192, 256) for q in range(4)], axis=1).astype(jnp.float32)
    quarters = mine.reshape(4, 48, 1024)
    picked = quarters[0]
    for k in range(1, 4):
        picked = jnp.where(m == k, quarters[k], picked)
    text = txt[own_text].reshape(48, 1024).astype(jnp.float32)
    factor = lax.rsqrt(jnp.sum(picked * picked, axis=1, keepdims=True) + 1e-6) * scale
    matched = factor * jnp.sum(picked * text, axis=1, keepdims=True)
    square = jnp.concatenate([jnp.broadcast_to(matched, (48, 128)), jnp.zeros((80, 128), jnp.float32)], axis=0)
    matched_lanes = jnp.transpose(square)[0:1, :]

    def waits(buf, send, recv, count):
        for n in range(1, count):
            pltpu.make_async_remote_copy(
                src_ref=buf.at[n], dst_ref=buf.at[n], send_sem=send.at[n], recv_sem=recv.at[n],
                device_id={"c": other}, device_id_type=pl.DeviceIdType.MESH,
            ).wait_recv()

    def merged(buf):
        states = buf[...]
        tops, totals = states[:, 0:1, :], states[:, 1:2, :]
        peak = jnp.max(tops, axis=0)
        return (peak + jnp.log2(jnp.sum(totals * jnp.exp2(tops - peak[None]), axis=0))) * LN2

    waits(cr, c_send, c_recv, 16)
    fin_src[0:1, :] = merged(cr)
    fin_src[1:2, :] = matched_lanes
    fin[m] = fin_src[...]
    lasts = []
    for n, (dz, dc) in enumerate(mp_peers):
        lasts.append(push(fin_src, fin.at[m], f_send.at[n], f_recv.at[n], mp_of(dz, dc)))
    waits(rr, r_send, r_recv, 32)
    row_lse = merged(rr)
    row_lse = jnp.where(odd == 0, row_lse, pltpu.roll(row_lse, 192, 1))[:, :256]
    for last in lasts:
        last.wait_recv()
    lane = lax.broadcasted_iota(jnp.int32, (1, 256), 1)
    whole = []
    for k in range(2):
        joined = jnp.zeros((1, 256), jnp.float32)
        for q in range(4):
            part = jnp.concatenate([fin[q, pl.ds(k, 1), :], jnp.zeros((1, 128), jnp.float32)], axis=1)
            part = pltpu.roll(part, q * 48, 1) if q else part
            joined = jnp.where((lane >= q * 48) & (lane < q * 48 + 48), part, joined)
        whole.append(joined)
    row_ref[...] = row_lse - whole[1]
    col_ref[...] = whole[0] - whole[1]
    for copy in started:
        copy.wait_send()


def on_device(images, texts, logit_scale):
    any_space = pl.BlockSpec(memory_space=pl.ANY)
    vmem = pl.BlockSpec(memory_space=pltpu.VMEM)
    dma = pltpu.SemaphoreType.DMA
    bf16, f32 = jnp.bfloat16, jnp.float32
    n_in, n_all = len(ITEMS), len(ALL)
    row, col = pl.pallas_call(
        body,
        out_shape=(jax.ShapeDtypeStruct((1, 256), f32), jax.ShapeDtypeStruct((1, 256), f32)),
        in_specs=[any_space, any_space, pl.BlockSpec(memory_space=pltpu.SMEM)],
        out_specs=(vmem, vmem),
        scratch_shapes=[
            pltpu.VMEM((8, 4, CHUNKS, 64, 256), bf16),
            pltpu.VMEM((16, CHUNKS, 16, 1024), bf16),
            pltpu.VMEM((4, 48, 256), bf16),
            pltpu.VMEM((4, 48, 256), bf16),
            pltpu.VMEM((1536, 128), f32),
            pltpu.VMEM((4, 2, 384), f32),
            pltpu.VMEM((32, 2, 384), f32),
            pltpu.VMEM((16, 2, 128), f32),
            pltpu.VMEM((16, 2, 128), f32),
            pltpu.VMEM((2, 128), f32),
            pltpu.VMEM((4, 2, 128), f32),
            dma((3,)),
            dma((3,)), dma((3,)),
            dma((n_in,)), dma((n_in,)),
            dma((n_in,)), dma((n_in,)),
            dma((n_all,)), dma((n_all,)),
            dma((32,)), dma((32,)),
            dma((16,)), dma((16,)),
            dma((3,)), dma((3,)),
        ],
        compiler_params=pltpu.CompilerParams(collective_id=0, has_side_effects=True),
        name="contrastive",
    )(images.reshape(CHUNKS, 64, 256), texts.reshape(4, 48, 256), logit_scale)
    return row[0, :192], col[0, :192]


def solution(mesh):
    finer = Mesh(mesh.devices.reshape(SIZES), AXES)
    return jax.shard_map(
        on_device,
        mesh=finer,
        in_specs=(P(("zl", "x", "y"), ("zh", "c")), P(("zl", "x", "y"), ("zh", "c")), P()),
        out_specs=(P(("zl", "x", "y")), P(("zl", "x", "y"))),
        check_vma=False,
    )
```

```python
import heapq

import jax
import jax.numpy as jnp
from jax import lax
from jax.experimental import pallas as pl
from jax.experimental.pallas import tpu as pltpu
from jax.sharding import Mesh
from jax.sharding import PartitionSpec as P

AXES = ("zl", "x", "y", "zh", "c")
SIZES = (4, 4, 8, 2, 2)
RING = 8
LOG2E = 1.4426950408889634
LN2 = 0.6931471805599453

PLACES = [(col, d) for col in (0, 1) for d in range(-3, 5)]
ROOT = PLACES.index((0, 0))
IMAGE_TREES = (
    (2, 0, 3, 3, 11, 4, 14, 0, 9, 10, 2, 3, 4, 11, 13, 14),
    (8, 9, 1, 3, 11, 3, 5, 6, 9, 11, 9, 3, 11, 5, 6, 8),
    (1, 3, 10, 3, 12, 13, 7, 1, 9, 1, 3, 3, 3, 12, 13, 7),
)
TEXT_TREES = (
    (8, 3, 3, 3, 3, 4, 14, 15, 1, 10, 2, 3, 13, 14, 3, 14),
    (8, 3, 3, 3, 3, 3, 5, 5, 9, 3, 11, 3, 4, 5, 13, 8),
    (1, 3, 3, 3, 3, 4, 5, 15, 15, 1, 2, 3, 3, 5, 4, 14),
    (8, 3, 3, 3, 3, 4, 5, 1, 1, 1, 2, 3, 13, 11, 13, 9),
    (2, 2, 3, 3, 12, 3, 5, 0, 9, 1, 2, 3, 11, 5, 6, 13),
    (1, 3, 1, 3, 3, 13, 7, 1, 0, 1, 9, 3, 4, 3, 12, 7),
)
IMAGE_KINDS = [(0.0, 0.7)] * 3
TEXT_KINDS = [(1.5, 0.35)] * 3 + [(5.5, 0.35)] * 3
BASE, MORE, FAR, BESIDE, TILE = 2.35, 0.85, 0.5, 2.0, 0.6


def path_of(parent, child):
    (pc, pd), (cc, cd) = PLACES[parent], PLACES[child]
    up = (cd - pd + RING) % RING
    up = up - RING if up > RING // 2 else up
    return (["across"] if pc != cc else []) + (["up"] * up if up > 0 else ["down"] * -up)


def delay_of(path):
    return BASE + MORE * (len(path) - 1) + FAR * (len(path) - path.count("across"))


def plan(trees, kinds, busy):
    free = {"up": busy, "down": busy, "across": 0.0}
    below, weight = [], []
    for kind, tree in enumerate(trees):
        kids = {p: [q for q in range(16) if q != ROOT and tree[q] == p] for p in range(16)}
        deep = {}

        def measure(p):
            deep[p] = max([0.0] + [delay_of(path_of(p, q)) + kinds[kind][1] + measure(q) for q in kids[p]])
            return deep[p]

        measure(ROOT)
        below.append({p: sorted(qs, key=lambda q: -deep[q]) for p, qs in kids.items()})
        weight.append(deep)
    heap = [(kinds[k][0], -weight[k][ROOT], k, ROOT) for k in range(len(trees))]
    heapq.heapify(heap)
    out = []
    while heap:
        t, _, kind, place = heapq.heappop(heap)
        out.append((t, kind, place, below[kind][place]))
        for child in below[kind][place]:
            path = path_of(place, child)
            begin = max(t, free[path[0]])
            ready = begin
            for link in sorted(set(path)):
                first = max(free[link], begin)
                free[link] = first + kinds[kind][1] * path.count(link)
                ready = max(ready, first + kinds[kind][1])
            heapq.heappush(heap, (ready + delay_of(path), -weight[kind][child], kind, child))
    return out


def timeline():
    images, texts = plan(IMAGE_TREES, IMAGE_KINDS, 2.0), plan(TEXT_TREES, TEXT_KINDS, 0.0)
    steps = [(t, "image", kind, place, kids) for t, kind, place, kids in images]
    steps += [(t, "text", kind, place, kids) for t, kind, place, kids in texts]
    image_at = [max(t for t, kind, _, _ in images if kind == k) + BESIDE for k in range(3)]
    text_at = [max(t for t, kind, _, _ in texts if kind % 3 == k) for k in range(3)]
    work = [(t, 0, "rows", i, 0) for i, t in enumerate(image_at)] + [(t, 1, "columns", k, 0) for k, t in enumerate(text_at)]
    work += [(max(image_at[i], text_at[k]), 2, "tile", i, k) for i in range(3) for k in range(3)]
    work += [(max(image_at), 3, "matched", 0, 0)]
    clock = 0.0
    for t, _, what, i, k in sorted(work):
        clock = max(clock, t)
        steps.append((clock, what, i, k, []))
        clock += TILE if what == "tile" else 0.3
    return sorted(steps, key=lambda s: s[0])


STEPS = timeline()


def body(
    images_ref, texts_ref, scale_ref, row_ref, col_ref,
    img, txt, tq, unit, fac, top, total, rs, rr, cs, cr, fin,
    load_sem, a_send, a_recv, i_send, i_recv, t_send, t_recv, d_send, d_recv,
    r_send, r_recv, c_send, c_recv, f_send, f_recv,
):
    zl, x, y, zh, c = (lax.axis_index(a) for a in AXES)
    z = zh * 4 + zl
    m = zh * 2 + c
    odd = lax.rem(x, 2)
    even = 1 - odd
    xf = x + 1 - 2 * odd
    xg = lax.rem(x + 3 + 2 * odd, 4)
    other = 1 - c
    zs = [lax.rem(z + d, RING) for d in range(RING)]
    ys = [lax.rem(y + d, RING) for d in range(RING)]
    z_of = [{"zl": lax.rem(p, 4), "zh": lax.div(p, 4)} for p in zs]
    own_block = zl * 2 + odd
    own_text = y * 2 + even
    loads = [
        pltpu.make_async_copy(texts_ref, tq, load_sem.at[0]),
        pltpu.make_async_copy(texts_ref.at[m], txt.at[own_text, m], load_sem.at[1]),
        pltpu.make_async_copy(images_ref, img.at[own_block, m], load_sem.at[2]),
    ]
    for load in loads:
        load.start()

    mp_peers = [(0, 1), (1, 0), (1, 1)]

    def mp_of(dz, dc):
        return {"zh": (1 - zh) if dz else zh, "c": other if dc else c}

    def hops(trees):
        seen = set()
        for tree in trees:
            for q in range(16):
                if q != ROOT:
                    (pc, pd), (cc, cd) = PLACES[tree[q]], PLACES[q]
                    step = ((cd - pd) % RING, int(pc != cc))
                    seen |= {step, ((-step[0]) % RING, step[1])}
        return sorted(seen)

    def image_peer(step):
        return {**z_of[step[0]], "x": xf if step[1] else x}

    def text_peer(step):
        return {"y": ys[step[0]], "x": xg if step[1] else x}

    peers = [image_peer(s) for s in hops(IMAGE_TREES)] + [text_peer(s) for s in hops(TEXT_TREES)]
    peers += [mp_of(*p) for p in mp_peers if p != (1, 0) or (4, 0) not in hops(IMAGE_TREES)]
    barrier = pltpu.get_barrier_semaphore()
    for peer in peers:
        pl.semaphore_signal(barrier, inc=1, device_id=peer, device_id_type=pl.DeviceIdType.MESH)
    for load in loads:
        load.wait()
    pl.semaphore_wait(barrier, len(peers))

    started = []

    def push(src, dst, send, recv, n, peer):
        copy = pltpu.make_async_remote_copy(
            src_ref=src, dst_ref=dst, send_sem=send.at[n], recv_sem=recv.at[n],
            device_id=peer, device_id_type=pl.DeviceIdType.MESH,
        )
        copy.start()
        started.append(copy)

    def arrived(buf, send, recv, n):
        pltpu.make_async_remote_copy(
            src_ref=buf, dst_ref=buf, send_sem=send.at[n], recv_sem=recv.at[n],
            device_id={"c": other}, device_id_type=pl.DeviceIdType.MESH,
        ).wait_recv()

    for n in (1, 2, 0):
        peer = mp_of(*mp_peers[n])
        push(tq.at[peer["zh"] * 2 + peer["c"]], txt.at[own_text, m], a_send, a_recv, n, peer)

    def image_slot(kind, place, core):
        col, d = PLACES[place]
        pos = z_of[-d % RING]
        return img.at[pos["zl"] * 2 + (even if col else odd), pos["zh"] * 2 + core, kind]

    def text_slot(kind, place):
        col, d = PLACES[place]
        half = zh if kind < 3 else 1 - zh
        return txt.at[ys[-d % RING] * 2 + (odd if col else even), pl.ds(half * 2, 2), kind % 3]

    def step_to(place, child):
        (pc, pd), (cc, cd) = PLACES[place], PLACES[child]
        return ((cd - pd) % RING, int(pc != cc))

    def image_step(kind, place, kids):
        slot = image_slot(kind, place, c)
        if place != ROOT:
            arrived(slot, i_send, i_recv, kind * 16 + place)
        for kid in kids:
            push(slot, slot, i_send, i_recv, kind * 16 + kid, image_peer(step_to(place, kid)))
        push(slot, slot, d_send, d_recv, kind * 16 + place, {"c": other})

    swapped = set()

    def text_step(kind, place, kids):
        slot = text_slot(kind, place)
        if place != ROOT:
            arrived(slot, t_send, t_recv, kind * 16 + place)
        else:
            for n in {0, 1, 2} - swapped if kind >= 3 else {0} - swapped:
                peer = mp_of(*mp_peers[n])
                arrived(txt.at[own_text, peer["zh"] * 2 + peer["c"]], a_send, a_recv, n)
                swapped.add(n)
        for kid in kids:
            push(slot, slot, t_send, t_recv, kind * 16 + kid, text_peer(step_to(place, kid)))

    scale = scale_ref[0]

    def rows_of(i):
        return jnp.concatenate([img[:, q, i].reshape(512, 256) for q in range(4)], axis=1)

    def rows_step(i):
        for place in range(16):
            arrived(image_slot(i, place, other), d_send, d_recv, i * 16 + place)
        wide = rows_of(i).astype(jnp.float32)
        factor = lax.rsqrt(jnp.sum(wide * wide, axis=1, keepdims=True) + 1e-6) * (scale * LOG2E)
        fac[i] = jnp.broadcast_to(factor, (512, 128))

    def columns_step(k):
        wide = jnp.concatenate([txt[:, q, k].reshape(256, 256) for q in range(4)], axis=1).astype(jnp.float32)
        wide = wide * lax.rsqrt(jnp.sum(wide * wide, axis=1, keepdims=True) + 1e-6)
        unit[k] = wide.astype(jnp.bfloat16)

    columns = {}
    seen_rows = set()

    def tile_step(i, k):
        dots = lax.dot_general(rows_of(i), unit[k], (((1,), (1,)), ((), ())), preferred_element_type=jnp.float32)
        factor = fac[i]
        scores = dots * jnp.concatenate([factor, factor], axis=1)
        row_top = jnp.max(scores, axis=1, keepdims=True)
        col_top = jnp.max(scores, axis=0, keepdims=True)
        if i in seen_rows:
            old = top[i]
            new = jnp.maximum(old, row_top)
            part = jnp.sum(jnp.exp2(scores - jnp.concatenate([new, new], axis=1)), axis=1, keepdims=True)
            total[i] = total[i] * jnp.exp2(old - new) + part
        else:
            new = jnp.broadcast_to(row_top, (512, 128))
            part = jnp.sum(jnp.exp2(scores - row_top), axis=1, keepdims=True)
            total[i] = jnp.broadcast_to(part, (512, 128))
        top[i] = new
        seen_rows.add(i)
        if k in columns:
            col_old, col_sum = columns[k]
            col_new = jnp.maximum(col_old, col_top)
            part = jnp.sum(jnp.exp2(scores - col_new), axis=0, keepdims=True)
            columns[k] = (col_new, col_sum * jnp.exp2(col_old - col_new) + part)
        else:
            columns[k] = (col_top, jnp.sum(jnp.exp2(scores - col_top), axis=0, keepdims=True))

    def matched_step():
        got = []
        for g in range(3):
            at = m * 3 + g
            chunk, row = lax.div(at, 4), pl.multiple_of(lax.rem(at, 4) * 16, 16)
            rows = [img[own_block, q, chunk, pl.ds(row, 16), :] for q in range(4)]
            rows = jnp.concatenate(rows, axis=1).astype(jnp.float32)
            text = jnp.concatenate([txt[own_text, q, g] for q in range(4)], axis=1).astype(jnp.float32)
            norms = [lax.rsqrt(jnp.sum(v * v, axis=1, keepdims=True) + 1e-6) for v in (rows, text)]
            got.append(jnp.sum(rows * text, axis=1, keepdims=True) * norms[0] * norms[1] * scale)
        tall = jnp.broadcast_to(jnp.concatenate(got, axis=0), (48, 128))
        square = jnp.concatenate([tall, jnp.zeros((80, 128), jnp.float32)], axis=0)
        fin[m] = jnp.transpose(square)[0:1, :]
        for n in (1, 2, 0):
            push(fin.at[m], fin.at[m], f_send, f_recv, n, mp_of(*mp_peers[n]))

    for _, what, a, b, kids in STEPS:
        if what == "image":
            image_step(a, b, kids)
        elif what == "text":
            text_step(a, b, kids)
        elif what == "rows":
            rows_step(a)
        elif what == "columns":
            columns_step(a)
        elif what == "tile":
            tile_step(a, b)
        else:
            matched_step()

    lane = lax.broadcasted_iota(jnp.int32, (2, 128), 1)
    states = [jnp.concatenate(columns[k], axis=0) for k in range(3)]
    for tb in range(16):
        turned = []
        for k in range(3):
            shift = (256 - tb * 16 + k * 16) % 256
            turned.append((pltpu.roll(states[k], shift, 1) if shift else states[k])[:, :128])
        cs[tb] = jnp.where(lane < 16, turned[0], jnp.where(lane < 32, turned[1], turned[2]))
    for dy in (4, 3, 5, 2, 6, 1, 7, 0):
        for dx in (1, 0):
            for dz, dc in ((1, 1), (1, 0), (0, 1), (0, 0)):
                n = ((dy * 2 + dx) * 2 + dz) * 2 + dc
                source = cs.at[ys[dy] * 2 + (odd if dx else even)]
                if n == 0:
                    cr[m, 0] = source[...]
                else:
                    peer = {**mp_of(dz, dc), "y": ys[dy], "x": xg if dx else x}
                    push(source, cr.at[m, dy * 2 + dx], c_send, c_recv, n, peer)
    lane = lax.broadcasted_iota(jnp.int32, (128, 128), 1)
    for i in range(3):
        for p in range(4):
            rows = pl.ds(p * 128, 128)
            rs[p, i] = jnp.transpose(jnp.where(lane == 0, top[i, rows, :], total[i, rows, :]))[0:2, :]
    for dz in (4, 3, 5, 2, 6, 1, 7, 0):
        for dx in (1, 0):
            for dc in (1, 0):
                n = dz * 4 + dx * 2 + dc
                if n == 0:
                    rr[0] = rs[zl]
                else:
                    peer = {**z_of[dz], "x": xf if dx else x, "c": other if dc else c}
                    push(rs.at[z_of[dz]["zl"]], rr.at[n], r_send, r_recv, n, peer)

    def merged(states):
        tops, totals = states[..., 0:1, :], states[..., 1:2, :]
        peak = jnp.max(tops, axis=0)
        return (peak + jnp.log2(jnp.sum(totals * jnp.exp2(tops - peak[None]), axis=0))) * LN2

    def placed(parts):
        lane = lax.broadcasted_iota(jnp.int32, (1, 256), 1)
        joined = jnp.zeros((1, 256), jnp.float32)
        for q, part in enumerate(parts):
            part = jnp.concatenate([part, jnp.zeros((1, 128), jnp.float32)], axis=1)
            part = pltpu.roll(part, q * 48, 1) if q else part
            joined = jnp.where((lane >= q * 48) & (lane < q * 48 + 48), part, joined)
        return joined

    for n in range(3):
        peer = mp_of(*mp_peers[n])
        arrived(fin.at[peer["zh"] * 2 + peer["c"]], f_send, f_recv, n)
    matched = placed([fin[q] for q in range(4)])
    for n in range(1, 32):
        arrived(rr.at[n], r_send, r_recv, n)
    lse = merged(rr[...])
    lane = lax.broadcasted_iota(jnp.int32, (1, 128), 1)
    kept = [jnp.where(odd == 0, lse[i], pltpu.roll(lse[i], 64, 1)) for i in range(3)]
    front = jnp.where(lane < 64, kept[0], pltpu.roll(kept[1], 64, 1))
    row_ref[...] = jnp.concatenate([front, kept[2]], axis=1) - matched
    for n in range(1, 64):
        dz, dc = (n // 2) % 2, n % 2
        peer = mp_of(dz, dc)
        arrived(cr.at[peer["zh"] * 2 + peer["c"], n // 4], c_send, c_recv, n)
    col_ref[...] = placed([merged(cr[q]) for q in range(4)]) - matched
    for copy in started:
        copy.wait_send()


def on_device(images, texts, logit_scale):
    any_space = pl.BlockSpec(memory_space=pl.ANY)
    vmem = pl.BlockSpec(memory_space=pltpu.VMEM)
    dma = pltpu.SemaphoreType.DMA
    bf16, f32 = jnp.bfloat16, jnp.float32
    row, col = pl.pallas_call(
        body,
        out_shape=(jax.ShapeDtypeStruct((1, 256), f32), jax.ShapeDtypeStruct((1, 256), f32)),
        in_specs=[any_space, any_space, pl.BlockSpec(memory_space=pltpu.SMEM)],
        out_specs=(vmem, vmem),
        scratch_shapes=[
            pltpu.VMEM((8, 4, 3, 64, 256), bf16),
            pltpu.VMEM((16, 4, 3, 16, 256), bf16),
            pltpu.VMEM((4, 3, 16, 256), bf16),
            pltpu.VMEM((3, 256, 1024), bf16),
            pltpu.VMEM((3, 512, 128), f32),
            pltpu.VMEM((3, 512, 128), f32),
            pltpu.VMEM((3, 512, 128), f32),
            pltpu.VMEM((4, 3, 2, 128), f32),
            pltpu.VMEM((32, 3, 2, 128), f32),
            pltpu.VMEM((16, 2, 128), f32),
            pltpu.VMEM((4, 16, 2, 128), f32),
            pltpu.VMEM((4, 1, 128), f32),
            dma((3,)),
            dma((3,)), dma((3,)),
            dma((48,)), dma((48,)),
            dma((96,)), dma((96,)),
            dma((48,)), dma((48,)),
            dma((32,)), dma((32,)),
            dma((64,)), dma((64,)),
            dma((3,)), dma((3,)),
        ],
        compiler_params=pltpu.CompilerParams(collective_id=0, has_side_effects=True),
        name="contrastive",
    )(images.reshape(3, 64, 256), texts.reshape(4, 3, 16, 256), logit_scale)
    return row[0, :192], col[0, :192]


def solution(mesh):
    finer = Mesh(mesh.devices.reshape(SIZES), AXES)
    return jax.shard_map(
        on_device,
        mesh=finer,
        in_specs=(P(("zl", "x", "y"), ("zh", "c")), P(("zl", "x", "y"), ("zh", "c")), P()),
        out_specs=(P(("zl", "x", "y")), P(("zl", "x", "y"))),
        check_vma=False,
    )
```

```python
import heapq

import jax
import jax.numpy as jnp
from jax import lax
from jax.experimental import pallas as pl
from jax.experimental.pallas import tpu as pltpu
from jax.sharding import Mesh
from jax.sharding import PartitionSpec as P

AXES = ("zl", "x", "y", "zh", "c")
SIZES = (4, 4, 8, 2, 2)
RING = 8
LOG2E = 1.4426950408889634
LN2 = 0.6931471805599453

PLACES = [(col, d) for col in (0, 1) for d in range(-3, 5)]
ROOT = PLACES.index((0, 0))
IMAGE_TREES = (
    (1, 2, 3, 3, 5, 6, 3, 15, 15, 1, 2, 3, 11, 5, 6, 6),
    (9, 2, 3, 3, 11, 4, 5, 1, 9, 1, 2, 3, 11, 12, 13, 7),
    (3, 0, 10, 3, 11, 4, 0, 6, 0, 10, 11, 3, 11, 12, 6, 8),
)
TEXT_TREES = (
    (3, 3, 3, 3, 3, 3, 5, 6, 15, 1, 11, 3, 3, 3, 6, 0),
    (3, 2, 10, 3, 5, 12, 7, 0, 0, 10, 3, 3, 11, 3, 13, 7),
    (1, 3, 10, 3, 3, 3, 5, 0, 0, 1, 3, 3, 4, 5, 8, 7),
    (2, 0, 3, 3, 11, 3, 5, 6, 15, 10, 11, 3, 4, 5, 6, 5),
    (1, 3, 10, 3, 3, 4, 3, 6, 0, 0, 11, 3, 4, 12, 6, 14),
    (1, 3, 1, 3, 12, 13, 7, 1, 9, 1, 2, 3, 3, 12, 12, 9),
)
IMAGE_KINDS = [(0.0, 0.7)] * 3
TEXT_KINDS = [(1.5, 0.35)] * 3 + [(6.5, 0.35)] * 3
BASE, MORE, FAR, BESIDE, TILE, LATE = 3.0, 0.5, 0.0, 2.0, 0.6, 0.8


def path_of(parent, child):
    (pc, pd), (cc, cd) = PLACES[parent], PLACES[child]
    up = (cd - pd + RING) % RING
    up = up - RING if up > RING // 2 else up
    return (["across"] if pc != cc else []) + (["up"] * up if up > 0 else ["down"] * -up)


def delay_of(path):
    return BASE + MORE * (len(path) - 1) + FAR * (len(path) - path.count("across"))


def plan(trees, kinds, busy):
    free = {"up": busy, "down": busy, "across": 0.0}
    below, weight = [], []
    for kind, tree in enumerate(trees):
        kids = {p: [q for q in range(16) if q != ROOT and tree[q] == p] for p in range(16)}
        deep = {}

        def measure(p):
            deep[p] = max([0.0] + [delay_of(path_of(p, q)) + kinds[kind][1] + measure(q) for q in kids[p]])
            return deep[p]

        measure(ROOT)
        below.append({p: sorted(qs, key=lambda q: -deep[q]) for p, qs in kids.items()})
        weight.append(deep)
    heap = [(kinds[k][0], -weight[k][ROOT], k, ROOT) for k in range(len(trees))]
    heapq.heapify(heap)
    out = []
    while heap:
        t, _, kind, place = heapq.heappop(heap)
        out.append((t, kind, place, below[kind][place]))
        for child in below[kind][place]:
            path = path_of(place, child)
            begin = max(t, free[path[0]])
            ready = begin
            for link in sorted(set(path)):
                first = max(free[link], begin)
                free[link] = first + kinds[kind][1] * path.count(link)
                ready = max(ready, first + kinds[kind][1])
            heapq.heappush(heap, (ready + delay_of(path), -weight[kind][child], kind, child))
    return out


def timeline():
    images, texts = plan(IMAGE_TREES, IMAGE_KINDS, 2.0), plan(TEXT_TREES, TEXT_KINDS, 0.0)
    steps = [(t, "image", kind, place, kids) for t, kind, place, kids in images if kids]
    steps += [(t + LATE, "image", kind, place, kids) for t, kind, place, kids in images if not kids]
    steps += [(t, "text", kind, place, kids) for t, kind, place, kids in texts if kids]
    image_at = [max(t for t, kind, _, _ in images if kind == k) + BESIDE for k in range(3)]
    text_at = [max(t for t, kind, _, _ in texts if kind % 3 == k) for k in range(3)]
    work = [(t, 0, "rows", i, 0) for i, t in enumerate(image_at)] + [(t, 1, "columns", k, 0) for k, t in enumerate(text_at)]
    work += [(max(image_at[i], text_at[k]), 2, "tile", i, k) for i in range(3) for k in range(3)]
    work += [(max(image_at), 3, "matched", 0, 0)]
    clock = 0.0
    for t, _, what, i, k in sorted(work):
        clock = max(clock, t)
        steps.append((clock, what, i, k, []))
        clock += TILE if what == "tile" else 0.3
    return sorted(steps, key=lambda s: s[0])


STEPS = timeline()
TEXT_SEATS = {}
for kind, tree in enumerate(TEXT_TREES):
    for place in range(16):
        if place != ROOT and place in tree:
            TEXT_SEATS[kind, place] = len(TEXT_SEATS)
    TEXT_SEATS[kind, None] = len(TEXT_SEATS)
for kind, tree in enumerate(TEXT_TREES):
    for place in range(16):
        if place not in tree:
            TEXT_SEATS[kind, place] = TEXT_SEATS[kind, None]


def body(
    images_ref, texts_ref, scale_ref, row_ref, col_ref, matched_ref,
    img, txt, tq, unit, fac, top, total, rs, rr, cs, cr, fin,
    load_sem, done_sem, a_send, a_recv, i_send, i_recv, t_send, t_recv, d_send, d_recv,
    r_send, r_recv, c_send, c_recv, f_send, f_recv,
):
    zl, x, y, zh, c = (lax.axis_index(a) for a in AXES)
    z = zh * 4 + zl
    m = zh * 2 + c
    odd = lax.rem(x, 2)
    even = 1 - odd
    xf = x + 1 - 2 * odd
    xg = lax.rem(x + 3 + 2 * odd, 4)
    other = 1 - c
    zs = [lax.rem(z + d, RING) for d in range(RING)]
    ys = [lax.rem(y + d, RING) for d in range(RING)]
    z_of = [{"zl": lax.rem(p, 4), "zh": lax.div(p, 4)} for p in zs]
    own_block = zl * 2 + odd
    own_text = y * 2 + even
    loads = [
        pltpu.make_async_copy(texts_ref, tq, load_sem.at[0]),
        pltpu.make_async_copy(texts_ref.at[m], txt.at[own_text, m], load_sem.at[1]),
        pltpu.make_async_copy(images_ref, img.at[own_block, zh, c], load_sem.at[2]),
    ]
    for load in loads:
        load.start()

    mp_peers = [(0, 1), (1, 0), (1, 1)]

    def mp_of(dz, dc):
        return {"zh": (1 - zh) if dz else zh, "c": other if dc else c}

    def hops(trees):
        seen = set()
        for tree in trees:
            for q in range(16):
                if q != ROOT:
                    (pc, pd), (cc, cd) = PLACES[tree[q]], PLACES[q]
                    step = ((cd - pd) % RING, int(pc != cc))
                    seen |= {step, ((-step[0]) % RING, step[1])}
        return sorted(seen)

    def image_peer(step):
        return {**z_of[step[0]], "x": xf if step[1] else x}

    def text_peer(step):
        return {"y": ys[step[0]], "x": xg if step[1] else x}

    peers = [image_peer(s) for s in hops(IMAGE_TREES)] + [text_peer(s) for s in hops(TEXT_TREES)]
    peers += [mp_of(*p) for p in mp_peers if p != (1, 0) or (4, 0) not in hops(IMAGE_TREES)]
    barrier = pltpu.get_barrier_semaphore()
    for peer in peers:
        pl.semaphore_signal(barrier, inc=1, device_id=peer, device_id_type=pl.DeviceIdType.MESH)
    for load in loads:
        load.wait()
    pl.semaphore_wait(barrier, len(peers))

    def push(src, dst, send, recv, peer):
        pltpu.make_async_remote_copy(
            src_ref=src, dst_ref=dst, send_sem=send, recv_sem=recv,
            device_id=peer, device_id_type=pl.DeviceIdType.MESH,
        ).start()

    def arrived(buf, recv):
        pltpu.make_async_remote_copy(
            src_ref=buf, dst_ref=buf, send_sem=done_sem, recv_sem=recv,
            device_id={"c": other}, device_id_type=pl.DeviceIdType.MESH,
        ).wait_recv()

    def sent(buf, send):
        pltpu.make_async_remote_copy(
            src_ref=buf, dst_ref=buf, send_sem=send, recv_sem=done_sem,
            device_id={"c": other}, device_id_type=pl.DeviceIdType.MESH,
        ).wait_send()

    for n in (1, 2, 0):
        peer = mp_of(*mp_peers[n])
        push(tq.at[peer["zh"] * 2 + peer["c"]], txt.at[own_text, m], a_send, a_recv.at[n], peer)

    def image_slot(kind, place, core):
        col, d = PLACES[place]
        pos = z_of[-d % RING]
        return img.at[pos["zl"] * 2 + (even if col else odd), pos["zh"], core, kind]

    def text_slot(kind, place):
        col, d = PLACES[place]
        half = zh if kind < 3 else 1 - zh
        return txt.at[ys[-d % RING] * 2 + (odd if col else even), pl.ds(half * 2, 2), kind % 3]

    def step_to(place, child):
        (pc, pd), (cc, cd) = PLACES[place], PLACES[child]
        return ((cd - pd) % RING, int(pc != cc))

    def seat(place):
        return place - (place > ROOT)

    def image_step(kind, place, kids):
        slot = image_slot(kind, place, c)
        if place != ROOT:
            arrived(slot, i_recv.at[kind * 15 + seat(place)])
        for kid in kids:
            push(slot, slot, i_send.at[kind], i_recv.at[kind * 15 + seat(kid)], image_peer(step_to(place, kid)))
        push(slot, slot, d_send.at[kind], d_recv.at[kind], {"c": other})


    swapped = set()

    def text_step(kind, place, kids):
        slot = text_slot(kind, place)
        if place != ROOT:
            arrived(slot, t_recv.at[TEXT_SEATS[kind, place]])
        else:
            for n in {0, 1, 2} - swapped if kind >= 3 else {0} - swapped:
                peer = mp_of(*mp_peers[n])
                arrived(txt.at[own_text, peer["zh"] * 2 + peer["c"]], a_recv.at[n])
                swapped.add(n)
        for kid in kids:
            push(slot, slot, t_send.at[kind], t_recv.at[TEXT_SEATS[kind, kid]], text_peer(step_to(place, kid)))

    scale = scale_ref[0]

    def rows_of(i):
        return jnp.concatenate([img[:, q // 2, q % 2, i].reshape(512, 256) for q in range(4)], axis=1)

    def rows_step(i):
        arrived(img.at[:, :, other, i], d_recv.at[i])
        wide = rows_of(i).astype(jnp.float32)
        factor = lax.rsqrt(jnp.sum(wide * wide, axis=1, keepdims=True) + 1e-6) * (scale * LOG2E)
        fac[i] = jnp.broadcast_to(factor, (512, 128))

    def columns_step(k):
        for kind in (k, k + 3):
            leaves = sum(q not in TEXT_TREES[kind] for q in range(16))
            arrived(txt.at[pl.ds(0, leaves), pl.ds(0, 2), k], t_recv.at[TEXT_SEATS[kind, None]])
        wide = jnp.concatenate([txt[:, q, k].reshape(256, 256) for q in range(4)], axis=1).astype(jnp.float32)
        wide = wide * lax.rsqrt(jnp.sum(wide * wide, axis=1, keepdims=True) + 1e-6)
        unit[k] = wide.astype(jnp.bfloat16)

    columns = {}
    seen_rows = set()

    def tile_step(i, k):
        dots = lax.dot_general(rows_of(i), unit[k], (((1,), (1,)), ((), ())), preferred_element_type=jnp.float32)
        factor = fac[i]
        scores = dots * jnp.concatenate([factor, factor], axis=1)
        row_top = jnp.max(scores, axis=1, keepdims=True)
        col_top = jnp.max(scores, axis=0, keepdims=True)
        if i in seen_rows:
            old = top[i]
            new = jnp.maximum(old, row_top)
            part = jnp.sum(jnp.exp2(scores - jnp.concatenate([new, new], axis=1)), axis=1, keepdims=True)
            total[i] = total[i] * jnp.exp2(old - new) + part
        else:
            new = jnp.broadcast_to(row_top, (512, 128))
            part = jnp.sum(jnp.exp2(scores - row_top), axis=1, keepdims=True)
            total[i] = jnp.broadcast_to(part, (512, 128))
        top[i] = new
        seen_rows.add(i)
        if k in columns:
            col_old, col_sum = columns[k]
            col_new = jnp.maximum(col_old, col_top)
            part = jnp.sum(jnp.exp2(scores - col_new), axis=0, keepdims=True)
            columns[k] = (col_new, col_sum * jnp.exp2(col_old - col_new) + part)
        else:
            columns[k] = (col_top, jnp.sum(jnp.exp2(scores - col_top), axis=0, keepdims=True))

    def matched_step():
        got = []
        for g in range(3):
            at = m * 3 + g
            chunk, row = lax.div(at, 4), pl.multiple_of(lax.rem(at, 4) * 16, 16)
            rows = [img[own_block, q // 2, q % 2, chunk, pl.ds(row, 16), :] for q in range(4)]
            rows = jnp.concatenate(rows, axis=1).astype(jnp.float32)
            text = jnp.concatenate([txt[own_text, q, g] for q in range(4)], axis=1).astype(jnp.float32)
            norms = [lax.rsqrt(jnp.sum(v * v, axis=1, keepdims=True) + 1e-6) for v in (rows, text)]
            got.append(jnp.sum(rows * text, axis=1, keepdims=True) * norms[0] * norms[1] * scale)
        tall = jnp.broadcast_to(jnp.concatenate(got, axis=0), (48, 128))
        square = jnp.concatenate([tall, jnp.zeros((80, 128), jnp.float32)], axis=0)
        fin[m] = jnp.transpose(square)[0:1, :]
        for n in (1, 2, 0):
            push(fin.at[m], fin.at[m], f_send, f_recv.at[n], mp_of(*mp_peers[n]))

    for _, what, a, b, kids in STEPS:
        if what == "image":
            image_step(a, b, kids)
        elif what == "text":
            text_step(a, b, kids)
        elif what == "rows":
            rows_step(a)
        elif what == "columns":
            columns_step(a)
        elif what == "tile":
            tile_step(a, b)
        else:
            matched_step()

    lane = lax.broadcasted_iota(jnp.int32, (2, 128), 1)
    states = [jnp.concatenate(columns[k], axis=0) for k in range(3)]
    for tb in range(16):
        turned = []
        for k in range(3):
            shift = (256 - tb * 16 + k * 16) % 256
            turned.append((pltpu.roll(states[k], shift, 1) if shift else states[k])[:, :128])
        cs[tb] = jnp.where(lane < 16, turned[0], jnp.where(lane < 32, turned[1], turned[2]))
    for dy in (4, 3, 5, 2, 6, 1, 7, 0):
        for dx in (1, 0):
            for dz, dc in ((1, 1), (1, 0), (0, 1), (0, 0)):
                n = ((dy * 2 + dx) * 2 + dz) * 2 + dc
                source = cs.at[ys[dy] * 2 + (odd if dx else even)]
                if n == 0:
                    cr[m * 16] = source[...]
                else:
                    peer = {**mp_of(dz, dc), "y": ys[dy], "x": xg if dx else x}
                    push(source, cr.at[m * 16 + dy * 2 + dx], c_send, c_recv, peer)
    lane = lax.broadcasted_iota(jnp.int32, (128, 128), 1)
    for i in range(3):
        for p in range(4):
            rows = pl.ds(p * 128, 128)
            rs[p, i] = jnp.transpose(jnp.where(lane == 0, top[i, rows, :], total[i, rows, :]))[0:2, :]
    for dz in (4, 3, 5, 2, 6, 1, 7, 0):
        for dx in (1, 0):
            for dc in (1, 0):
                n = dz * 4 + dx * 2 + dc
                if n == 0:
                    rr[0] = rs[zl]
                else:
                    peer = {**z_of[dz], "x": xf if dx else x, "c": other if dc else c}
                    push(rs.at[z_of[dz]["zl"]], rr.at[n], r_send, r_recv, peer)

    for k in range(3):
        sent(img.at[pl.ds(0, 5), 0, 0], i_send.at[k])
        sent(img.at[:, :, 0, 0], d_send.at[k])
        for kind in (k, k + 3):
            sent(txt.at[pl.ds(0, 15), pl.ds(0, 2), 0], t_send.at[kind])
    sent(tq.at[pl.ds(0, 3)], a_send)
    sent(fin.at[pl.ds(0, 3)], f_send)

    def merged(states):
        tops, totals = states[..., 0:1, :], states[..., 1:2, :]
        peak = jnp.max(tops, axis=0)
        return (peak + jnp.log2(jnp.sum(totals * jnp.exp2(tops - peak[None]), axis=0))) * LN2

    def placed(parts):
        lane = lax.broadcasted_iota(jnp.int32, (1, 256), 1)
        joined = jnp.zeros((1, 256), jnp.float32)
        for q, part in enumerate(parts):
            part = jnp.concatenate([part, jnp.zeros((1, 128), jnp.float32)], axis=1)
            part = pltpu.roll(part, q * 48, 1) if q else part
            joined = jnp.where((lane >= q * 48) & (lane < q * 48 + 48), part, joined)
        return joined

    for n in range(3):
        peer = mp_of(*mp_peers[n])
        arrived(fin.at[peer["zh"] * 2 + peer["c"]], f_recv.at[n])
    matched = placed([fin[q] for q in range(4)])
    arrived(rr.at[pl.ds(1, 31)], r_recv)
    lse = merged(rr[...])
    lane = lax.broadcasted_iota(jnp.int32, (1, 128), 1)
    kept = [jnp.where(odd == 0, lse[i], pltpu.roll(lse[i], 64, 1)) for i in range(3)]
    front = jnp.where(lane < 64, kept[0], pltpu.roll(kept[1], 64, 1))
    row_ref[...] = jnp.concatenate([front, kept[2]], axis=1)
    matched_ref[...] = matched
    arrived(cr.at[pl.ds(1, 63)], c_recv)
    col_ref[...] = placed([merged(cr[pl.ds(q * 16, 16)]) for q in range(4)])
    sent(rr.at[pl.ds(1, 31)], r_send)
    sent(cr.at[pl.ds(1, 63)], c_send)


def on_device(images, texts, logit_scale):
    any_space = pl.BlockSpec(memory_space=pl.ANY)
    vmem = pl.BlockSpec(memory_space=pltpu.VMEM)
    dma = pltpu.SemaphoreType.DMA
    bf16, f32 = jnp.bfloat16, jnp.float32
    row, col, matched = pl.pallas_call(
        body,
        out_shape=(jax.ShapeDtypeStruct((1, 256), f32),) * 3,
        in_specs=[any_space, any_space, pl.BlockSpec(memory_space=pltpu.SMEM)],
        out_specs=(vmem,) * 3,
        scratch_shapes=[
            pltpu.VMEM((8, 2, 2, 3, 64, 256), bf16),
            pltpu.VMEM((16, 4, 3, 16, 256), bf16),
            pltpu.VMEM((4, 3, 16, 256), bf16),
            pltpu.VMEM((3, 256, 1024), bf16),
            pltpu.VMEM((3, 512, 128), f32),
            pltpu.VMEM((3, 512, 128), f32),
            pltpu.VMEM((3, 512, 128), f32),
            pltpu.VMEM((4, 3, 2, 128), f32),
            pltpu.VMEM((32, 3, 2, 128), f32),
            pltpu.VMEM((16, 2, 128), f32),
            pltpu.VMEM((64, 2, 128), f32),
            pltpu.VMEM((4, 1, 128), f32),
            dma((3,)), dma(()),
            dma(()), dma((3,)),
            dma((3,)), dma((45,)),
            dma((6,)), dma((max(TEXT_SEATS.values()) + 1,)),
            dma((3,)), dma((3,)),
            dma(()), dma(()),
            dma(()), dma(()),
            dma(()), dma((3,)),
        ],
        compiler_params=pltpu.CompilerParams(collective_id=0, has_side_effects=True),
        name="contrastive",
    )(images.reshape(3, 64, 256), texts.reshape(4, 3, 16, 256), logit_scale)
    return (row - matched)[0, :192], (col - matched)[0, :192]


def solution(mesh):
    finer = Mesh(mesh.devices.reshape(SIZES), AXES)
    return jax.shard_map(
        on_device,
        mesh=finer,
        in_specs=(P(("zl", "x", "y"), ("zh", "c")), P(("zl", "x", "y"), ("zh", "c")), P()),
        out_specs=(P(("zl", "x", "y")), P(("zl", "x", "y"))),
        check_vma=False,
    )
```

```python
import heapq

import jax
import jax.numpy as jnp
from jax import lax
from jax.experimental import pallas as pl
from jax.experimental.pallas import tpu as pltpu
from jax.sharding import Mesh
from jax.sharding import PartitionSpec as P

AXES = ("zl", "x", "y", "zh", "c")
SIZES = (4, 4, 8, 2, 2)
RING = 8
LOG2E = 1.4426950408889634
LN2 = 0.6931471805599453

PLACES = [(col, d) for col in (0, 1) for d in range(-3, 5)]
ROOT = PLACES.index((0, 0))
IMAGE_TREES = (
    (1, 2, 3, 3, 5, 6, 3, 15, 15, 1, 2, 3, 11, 5, 6, 6),
    (9, 2, 3, 3, 11, 4, 5, 1, 9, 1, 2, 3, 11, 12, 13, 7),
    (3, 0, 10, 3, 11, 4, 0, 6, 0, 10, 11, 3, 11, 12, 6, 8),
)
TEXT_TREES = (
    (3, 3, 3, 3, 3, 3, 5, 6, 15, 1, 11, 3, 3, 3, 6, 0),
    (3, 2, 10, 3, 5, 12, 7, 0, 0, 10, 3, 3, 11, 3, 13, 7),
    (1, 3, 10, 3, 3, 3, 5, 0, 0, 1, 3, 3, 4, 5, 8, 7),
    (2, 0, 3, 3, 11, 3, 5, 6, 15, 10, 11, 3, 4, 5, 6, 5),
    (1, 3, 10, 3, 3, 4, 3, 6, 0, 0, 11, 3, 4, 12, 6, 14),
    (1, 3, 1, 3, 12, 13, 7, 1, 9, 1, 2, 3, 3, 12, 12, 9),
)
IMAGE_KINDS = [(0.0, 0.7)] * 3
TEXT_KINDS = [(1.5, 0.35)] * 3 + [(6.5, 0.35)] * 3
BASE, MORE, FAR, BESIDE, TILE, LATE = 3.0, 0.5, 0.0, 2.0, 0.65, 0.8


def path_of(parent, child):
    (pc, pd), (cc, cd) = PLACES[parent], PLACES[child]
    up = (cd - pd + RING) % RING
    up = up - RING if up > RING // 2 else up
    return (["across"] if pc != cc else []) + (["up"] * up if up > 0 else ["down"] * -up)


def delay_of(path):
    return BASE + MORE * (len(path) - 1) + FAR * (len(path) - path.count("across"))


def plan(trees, kinds, busy):
    free = {"up": busy, "down": busy, "across": 0.0}
    below, weight = [], []
    for kind, tree in enumerate(trees):
        kids = {p: [q for q in range(16) if q != ROOT and tree[q] == p] for p in range(16)}
        deep = {}

        def measure(p):
            deep[p] = max([0.0] + [delay_of(path_of(p, q)) + kinds[kind][1] + measure(q) for q in kids[p]])
            return deep[p]

        measure(ROOT)
        below.append({p: sorted(qs, key=lambda q: -deep[q]) for p, qs in kids.items()})
        weight.append(deep)
    heap = [(kinds[k][0], -weight[k][ROOT], k, ROOT) for k in range(len(trees))]
    heapq.heapify(heap)
    out = []
    while heap:
        t, _, kind, place = heapq.heappop(heap)
        out.append((t, kind, place, below[kind][place]))
        for child in below[kind][place]:
            path = path_of(place, child)
            begin = max(t, free[path[0]])
            ready = begin
            for link in sorted(set(path)):
                first = max(free[link], begin)
                free[link] = first + kinds[kind][1] * path.count(link)
                ready = max(ready, first + kinds[kind][1])
            heapq.heappush(heap, (ready + delay_of(path), -weight[kind][child], kind, child))
    return out


def by_distance():
    last = {}
    for t, _, place, _ in plan(TEXT_TREES, TEXT_KINDS, 0.0):
        last[place] = max(t, last.get(place, 0.0))
    order = sorted(last, key=lambda place: last[place])
    return order[:8], order[8:]


NEAR_FAR = by_distance()


def timeline():
    images, texts = plan(IMAGE_TREES, IMAGE_KINDS, 2.0), plan(TEXT_TREES, TEXT_KINDS, 0.0)
    steps = [(t, "image", kind, place, kids) for t, kind, place, kids in images if kids]
    steps += [(t + LATE, "image", kind, place, kids) for t, kind, place, kids in images if not kids]
    steps += [(t, "text", kind, place, kids) for t, kind, place, kids in texts if kids]
    image_at = [max(t for t, kind, _, _ in images if kind == k) + BESIDE for k in range(3)]
    text_at = [max(t for t, _, place, _ in texts if place in group) for group in NEAR_FAR]
    work = [(t, 0, "rows", i, 0) for i, t in enumerate(image_at)]
    work += [(t, 1, "columns", g, 0) for g, t in enumerate(text_at)]
    work += [(max(image_at[i], text_at[g]), 2, "tile", i, g) for i in range(3) for g in range(2)]
    clock = 0.0
    for t, _, what, i, k in sorted(work):
        clock = max(clock, t)
        steps.append((clock, what, i, k, []))
        clock += TILE if what == "tile" else 0.3
    return sorted(steps, key=lambda s: s[0])


STEPS = timeline()
TEXT_SEATS, LEAVES = {}, {}
for kind, tree in enumerate(TEXT_TREES):
    for place in range(16):
        if place != ROOT and place in tree:
            TEXT_SEATS[kind, place] = len(TEXT_SEATS)
N_SEATS = len(TEXT_SEATS)
for kind, tree in enumerate(TEXT_TREES):
    for g, group in enumerate(NEAR_FAR):
        LEAVES[kind, g] = (N_SEATS, sum(place not in tree for place in group))
        for place in group:
            if place not in tree:
                TEXT_SEATS[kind, place] = N_SEATS
        N_SEATS += 1


def body(
    images_ref, texts_ref, scale_ref, row_ref, col_ref, matched_ref,
    img, txt, tq, unit, fac, held, rs, rr, cs, cr, fin,
    load_sem, done_sem, a_send, a_recv, i_send, i_recv, t_send, t_recv, d_send, d_recv,
    r_send, r_recv, c_send, c_recv, f_send, f_recv,
):
    zl, x, y, zh, c = (lax.axis_index(a) for a in AXES)
    z = zh * 4 + zl
    m = zh * 2 + c
    odd = lax.rem(x, 2)
    even = 1 - odd
    xf = x + 1 - 2 * odd
    xg = lax.rem(x + 3 + 2 * odd, 4)
    other = 1 - c
    zs = [lax.rem(z + d, RING) for d in range(RING)]
    ys = [lax.rem(y + d, RING) for d in range(RING)]
    z_of = [{"zl": lax.rem(p, 4), "zh": lax.div(p, 4)} for p in zs]
    own_block = zl * 2 + odd
    own_text = y * 2 + even
    loads = [
        pltpu.make_async_copy(texts_ref, tq, load_sem.at[0]),
        pltpu.make_async_copy(texts_ref.at[m], txt.at[own_text, m], load_sem.at[1]),
        pltpu.make_async_copy(images_ref, img.at[own_block, zh, c], load_sem.at[2]),
    ]
    for load in loads:
        load.start()

    mp_peers = [(0, 1), (1, 0), (1, 1)]

    def mp_of(dz, dc):
        return {"zh": (1 - zh) if dz else zh, "c": other if dc else c}

    def hops(trees):
        seen = set()
        for tree in trees:
            for q in range(16):
                if q != ROOT:
                    (pc, pd), (cc, cd) = PLACES[tree[q]], PLACES[q]
                    step = ((cd - pd) % RING, int(pc != cc))
                    seen |= {step, ((-step[0]) % RING, step[1])}
        return sorted(seen)

    def image_peer(step):
        return {**z_of[step[0]], "x": xf if step[1] else x}

    def text_peer(step):
        return {"y": ys[step[0]], "x": xg if step[1] else x}

    peers = [image_peer(s) for s in hops(IMAGE_TREES)] + [text_peer(s) for s in hops(TEXT_TREES)]
    peers += [mp_of(*p) for p in mp_peers if p != (1, 0) or (4, 0) not in hops(IMAGE_TREES)]
    barrier = pltpu.get_barrier_semaphore()
    for peer in peers:
        pl.semaphore_signal(barrier, inc=1, device_id=peer, device_id_type=pl.DeviceIdType.MESH)
    for load in loads:
        load.wait()
    pl.semaphore_wait(barrier, len(peers))

    def push(src, dst, send, recv, peer):
        pltpu.make_async_remote_copy(
            src_ref=src, dst_ref=dst, send_sem=send, recv_sem=recv,
            device_id=peer, device_id_type=pl.DeviceIdType.MESH,
        ).start()

    def arrived(buf, recv):
        pltpu.make_async_remote_copy(
            src_ref=buf, dst_ref=buf, send_sem=done_sem, recv_sem=recv,
            device_id={"c": other}, device_id_type=pl.DeviceIdType.MESH,
        ).wait_recv()

    def sent(buf, send):
        pltpu.make_async_remote_copy(
            src_ref=buf, dst_ref=buf, send_sem=send, recv_sem=done_sem,
            device_id={"c": other}, device_id_type=pl.DeviceIdType.MESH,
        ).wait_send()

    for n in (1, 2, 0):
        peer = mp_of(*mp_peers[n])
        push(tq.at[peer["zh"] * 2 + peer["c"]], txt.at[own_text, m], a_send, a_recv.at[n], peer)

    def image_slot(kind, place, core):
        col, d = PLACES[place]
        pos = z_of[-d % RING]
        return img.at[pos["zl"] * 2 + (even if col else odd), pos["zh"], core, kind]

    def text_slot(kind, place):
        col, d = PLACES[place]
        half = zh if kind < 3 else 1 - zh
        return txt.at[ys[-d % RING] * 2 + (odd if col else even), pl.ds(half * 2, 2), kind % 3]

    def step_to(place, child):
        (pc, pd), (cc, cd) = PLACES[place], PLACES[child]
        return ((cd - pd) % RING, int(pc != cc))

    def seat(place):
        return place - (place > ROOT)

    def image_step(kind, place, kids):
        slot = image_slot(kind, place, c)
        if place != ROOT:
            arrived(slot, i_recv.at[kind * 15 + seat(place)])
        for kid in kids:
            push(slot, slot, i_send.at[kind], i_recv.at[kind * 15 + seat(kid)], image_peer(step_to(place, kid)))
        push(slot, slot, d_send.at[kind], d_recv.at[kind], {"c": other})


    swapped = set()

    def text_step(kind, place, kids):
        slot = text_slot(kind, place)
        if place != ROOT:
            arrived(slot, t_recv.at[TEXT_SEATS[kind, place]])
        else:
            for n in {0, 1, 2} - swapped if kind >= 3 else {0} - swapped:
                peer = mp_of(*mp_peers[n])
                arrived(txt.at[own_text, peer["zh"] * 2 + peer["c"]], a_recv.at[n])
                swapped.add(n)
        for kid in kids:
            push(slot, slot, t_send.at[kind], t_recv.at[TEXT_SEATS[kind, kid]], text_peer(step_to(place, kid)))

    scale = scale_ref[0]

    def rows_of(i):
        return jnp.concatenate([img[:, q // 2, q % 2, i].reshape(512, 256) for q in range(4)], axis=1)

    def rows_step(i):
        arrived(img.at[:, :, other, i], d_recv.at[i])
        wide = rows_of(i).astype(jnp.float32)
        factor = lax.rsqrt(jnp.sum(wide * wide, axis=1, keepdims=True) + 1e-6) * (scale * LOG2E)
        fac[i] = jnp.broadcast_to(factor, (512, 128))

    def columns_step(g):
        for kind in range(6):
            seat, leaves = LEAVES[kind, g]
            if leaves:
                arrived(txt.at[pl.ds(0, leaves), pl.ds(0, 2), kind % 3], t_recv.at[seat])
        for j, place in enumerate(NEAR_FAR[g]):
            col, d = PLACES[place]
            at = ys[-d % RING] * 2 + (odd if col else even)
            wide = jnp.concatenate([txt[at, q].reshape(48, 256) for q in range(4)], axis=1).astype(jnp.float32)
            wide = wide * lax.rsqrt(jnp.sum(wide * wide, axis=1, keepdims=True) + 1e-6)
            unit[g, pl.ds(j * 48, 48), :] = wide.astype(jnp.bfloat16)

    columns = {}
    seen_rows = set()

    def tile_step(i, k):
        dots = lax.dot_general(rows_of(i), unit[k], (((1,), (1,)), ((), ())), preferred_element_type=jnp.float32)
        factor = fac[i]
        scores = dots * jnp.concatenate([factor] * 3, axis=1)
        row_top = jnp.max(scores, axis=1, keepdims=True)
        col_top = jnp.max(scores, axis=0, keepdims=True)
        row_total = jnp.sum(jnp.exp2(scores - row_top), axis=1, keepdims=True)
        lane = lax.broadcasted_iota(jnp.int32, (512, 128), 1)
        rest = jnp.where(lane == 2 * k + 1, row_total, held[i]) if i in seen_rows else row_total
        held[i] = jnp.where(lane == 2 * k, row_top, rest)
        seen_rows.add(i)
        if k in columns:
            col_old, col_sum = columns[k]
            col_new = jnp.maximum(col_old, col_top)
            part = jnp.sum(jnp.exp2(scores - col_new), axis=0, keepdims=True)
            columns[k] = (col_new, col_sum * jnp.exp2(col_old - col_new) + part)
        else:
            columns[k] = (col_top, jnp.sum(jnp.exp2(scores - col_top), axis=0, keepdims=True))

    def matched_step():
        got = []
        for g in range(3):
            at = m * 3 + g
            chunk, row = lax.div(at, 4), pl.multiple_of(lax.rem(at, 4) * 16, 16)
            rows = [img[own_block, q // 2, q % 2, chunk, pl.ds(row, 16), :] for q in range(4)]
            rows = jnp.concatenate(rows, axis=1).astype(jnp.float32)
            text = jnp.concatenate([txt[own_text, q, g] for q in range(4)], axis=1).astype(jnp.float32)
            norms = [lax.rsqrt(jnp.sum(v * v, axis=1, keepdims=True) + 1e-6) for v in (rows, text)]
            got.append(jnp.sum(rows * text, axis=1, keepdims=True) * norms[0] * norms[1] * scale)
        tall = jnp.broadcast_to(jnp.concatenate(got, axis=0), (48, 128))
        square = jnp.concatenate([tall, jnp.zeros((80, 128), jnp.float32)], axis=0)
        fin[m] = jnp.transpose(square)[0:1, :]
        for n in (1, 2, 0):
            push(fin.at[m], fin.at[m], f_send, f_recv.at[n], mp_of(*mp_peers[n]))

    for _, what, a, b, kids in STEPS:
        if what == "image":
            image_step(a, b, kids)
        elif what == "text":
            text_step(a, b, kids)
        elif what == "rows":
            rows_step(a)
        elif what == "columns":
            columns_step(a)
        else:
            tile_step(a, b)

    for g, group in enumerate(NEAR_FAR):
        states = jnp.concatenate(columns[g], axis=0)
        for j, place in enumerate(group):
            cs[place] = (pltpu.roll(states, 384 - j * 48, 1) if j else states)[:, :128]
    for dy in (4, 3, 5, 2, 6, 1, 7, 0):
        for dx in (1, 0):
            for dz, dc in ((1, 1), (1, 0), (0, 1), (0, 0)):
                n = ((dy * 2 + dx) * 2 + dz) * 2 + dc
                source = cs.at[PLACES.index((dx, 4 if dy == 4 else (-dy + 3) % RING - 3))]
                if n == 0:
                    cr[m * 16] = source[...]
                else:
                    peer = {**mp_of(dz, dc), "y": ys[dy], "x": xg if dx else x}
                    push(source, cr.at[m * 16 + dy * 2 + dx], c_send, c_recv, peer)
    for i in range(3):
        for p in range(4):
            turned = jnp.transpose(held[i, pl.ds(p * 128, 128), :])
            tops = [turned[2 * k : 2 * k + 1, :] for k in range(2)]
            peak = jnp.maximum(tops[0], tops[1])
            sums = [turned[2 * k + 1 : 2 * k + 2, :] * jnp.exp2(tops[k] - peak) for k in range(2)]
            rs[p, i, 0:1, :] = peak
            rs[p, i, 1:2, :] = sums[0] + sums[1]
    for dz in (4, 3, 5, 2, 6, 1, 7, 0):
        for dx in (1, 0):
            for dc in (1, 0):
                n = dz * 4 + dx * 2 + dc
                if n == 0:
                    rr[0] = rs[zl]
                else:
                    peer = {**z_of[dz], "x": xf if dx else x, "c": other if dc else c}
                    push(rs.at[z_of[dz]["zl"]], rr.at[n], r_send, r_recv, peer)

    matched_step()
    for k in range(3):
        sent(img.at[pl.ds(0, 5), 0, 0], i_send.at[k])
        sent(img.at[:, :, 0, 0], d_send.at[k])
        for kind in (k, k + 3):
            sent(txt.at[pl.ds(0, 15), pl.ds(0, 2), 0], t_send.at[kind])
    sent(tq.at[pl.ds(0, 3)], a_send)

    def merged(states):
        tops, totals = states[..., 0:1, :], states[..., 1:2, :]
        peak = jnp.max(tops, axis=0)
        return (peak + jnp.log2(jnp.sum(totals * jnp.exp2(tops - peak[None]), axis=0))) * LN2

    def placed(parts):
        lane = lax.broadcasted_iota(jnp.int32, (1, 256), 1)
        joined = jnp.zeros((1, 256), jnp.float32)
        for q, part in enumerate(parts):
            part = jnp.concatenate([part, jnp.zeros((1, 128), jnp.float32)], axis=1)
            part = pltpu.roll(part, q * 48, 1) if q else part
            joined = jnp.where((lane >= q * 48) & (lane < q * 48 + 48), part, joined)
        return joined

    arrived(rr.at[pl.ds(1, 31)], r_recv)
    lse = merged(rr[...])
    lane = lax.broadcasted_iota(jnp.int32, (1, 128), 1)
    kept = [jnp.where(odd == 0, lse[i], pltpu.roll(lse[i], 64, 1)) for i in range(3)]
    front = jnp.where(lane < 64, kept[0], pltpu.roll(kept[1], 64, 1))
    row_ref[...] = jnp.concatenate([front, kept[2]], axis=1)
    for n in range(3):
        peer = mp_of(*mp_peers[n])
        arrived(fin.at[peer["zh"] * 2 + peer["c"]], f_recv.at[n])
    matched = placed([fin[q] for q in range(4)])
    matched_ref[...] = matched
    arrived(cr.at[pl.ds(1, 63)], c_recv)
    col_ref[...] = placed([merged(cr[pl.ds(q * 16, 16)]) for q in range(4)])
    sent(rr.at[pl.ds(1, 31)], r_send)
    sent(cr.at[pl.ds(1, 63)], c_send)
    sent(fin.at[pl.ds(0, 3)], f_send)


def on_device(images, texts, logit_scale):
    any_space = pl.BlockSpec(memory_space=pl.ANY)
    vmem = pl.BlockSpec(memory_space=pltpu.VMEM)
    dma = pltpu.SemaphoreType.DMA
    bf16, f32 = jnp.bfloat16, jnp.float32
    row, col, matched = pl.pallas_call(
        body,
        out_shape=(jax.ShapeDtypeStruct((1, 256), f32),) * 3,
        in_specs=[any_space, any_space, pl.BlockSpec(memory_space=pltpu.SMEM)],
        out_specs=(vmem,) * 3,
        scratch_shapes=[
            pltpu.VMEM((8, 2, 2, 3, 64, 256), bf16),
            pltpu.VMEM((16, 4, 3, 16, 256), bf16),
            pltpu.VMEM((4, 3, 16, 256), bf16),
            pltpu.VMEM((2, 384, 1024), bf16),
            pltpu.VMEM((3, 512, 128), f32),
            pltpu.VMEM((3, 512, 128), f32),
            pltpu.VMEM((4, 3, 2, 128), f32),
            pltpu.VMEM((32, 3, 2, 128), f32),
            pltpu.VMEM((16, 2, 128), f32),
            pltpu.VMEM((64, 2, 128), f32),
            pltpu.VMEM((4, 1, 128), f32),
            dma((3,)), dma(()),
            dma(()), dma((3,)),
            dma((3,)), dma((45,)),
            dma((6,)), dma((N_SEATS,)),
            dma((3,)), dma((3,)),
            dma(()), dma(()),
            dma(()), dma(()),
            dma(()), dma((3,)),
        ],
        compiler_params=pltpu.CompilerParams(collective_id=0, has_side_effects=True),
        name="contrastive",
    )(images.reshape(3, 64, 256), texts.reshape(4, 3, 16, 256), logit_scale)
    return (row - matched)[0, :192], (col - matched)[0, :192]


def solution(mesh):
    finer = Mesh(mesh.devices.reshape(SIZES), AXES)
    return jax.shard_map(
        on_device,
        mesh=finer,
        in_specs=(P(("zl", "x", "y"), ("zh", "c")), P(("zl", "x", "y"), ("zh", "c")), P()),
        out_specs=(P(("zl", "x", "y")), P(("zl", "x", "y"))),
        check_vma=False,
    )
```
